32 devices in a mesh: seq: 8 (over z, y), tensor: 4 (over x, core).
Axes of the slice: x: 2, y: 2, z: 4, core: 2. Of those that a mesh axis runs over, the one named last changes fastest.
Arguments:
- hidden_in: bfloat16 [1024, 8192], P('seq', 'tensor'), may hold values from -6 to 6
- grad_out: bfloat16 [1024, 8192], P('seq', 'tensor'), may hold values from -6 to 6
- slot_tokens: int32 [128], P('seq'), may hold values from 0 to 127, as said below
- live_counts: int32 [8], P('seq'), may hold values from 5 to 16, as said below
- norm_gain: float32 [8192], P('tensor'), may hold values from 0.5 to 1.5
- router_weight: float32 [8192], P('tensor'), may hold values from -0.0625 to 0.0625
- gate_weight: bfloat16 [8192, 24576], P('tensor', 'seq'), may hold values from -0.0625 to 0.0625
- up_weight: bfloat16 [8192, 24576], P('tensor', 'seq'), may hold values from -0.0625 to 0.0625
- down_weight: bfloat16 [24576, 8192], P('seq', 'tensor'), may hold values from -0.0390625 to 0.0390625
Outputs:
- grad_in: bfloat16 [1024, 8192], P('seq', 'tensor')
- grad_gate: bfloat16 [8192, 24576], P('tensor', 'seq')
- grad_up: bfloat16 [8192, 24576], P('tensor', 'seq')
- grad_down: bfloat16 [24576, 8192], P('seq', 'tensor')
- grad_gain: float32 [8192], P('tensor')
- grad_router: float32 [8192], P('tensor')
The draws below stay inside these ranges and needn't reach their ends.
Inputs may be any that keep to these rules, and one draw needn't show every extreme that they name: `slot_tokens`: slot p belongs to index p // 16 of seq; the live slots of one index hold distinct positions, the others hold arbitrary positions of that index. `live_counts`: in every draw some index of seq has all 16 slots live.
All inputs are finite; a program needn't handle non-finite values.
Results may differ from the reference program's by a relative error of at most 0.0077.
Values may be sent and summed in bfloat16 or wider, within the bound.
A program may use at most 128 MiB of HBM per device.

```python
import jax
import jax.numpy as jnp
from jax import lax

D = 8192
FF = 24576
TOK_DEV = 128
CAP = 16
TOKENS = 1024
N_SEQ = 8


def routing_draw(key):
    base = jax.random.fold_in(key, 11)
    first, second, third, fourth = jax.random.split(base, 4)
    lowest = max(CAP // 3, 1)
    ranks = jnp.arange(N_SEQ, dtype=jnp.int32)
    floors = lowest + (CAP - lowest) * ranks // max(N_SEQ - 1, 1)
    counts = jax.random.randint(first, (N_SEQ,), floors, CAP + 1, dtype=jnp.int32)
    chosen = jax.random.randint(second, (), 0, N_SEQ, dtype=jnp.int32)
    counts = jnp.where(ranks == chosen, CAP, counts).astype(jnp.int32)
    keys = jax.random.split(third, N_SEQ)
    orders = jax.vmap(lambda single: jax.random.permutation(single, TOK_DEV))(keys)[:, :CAP].astype(jnp.int32)
    filler = jax.random.randint(fourth, (N_SEQ, CAP), 0, TOK_DEV, dtype=jnp.int32)
    columns = jnp.arange(CAP, dtype=jnp.int32)[None, :]
    tokens = jnp.where(columns < counts[:, None], orders, filler).reshape(-1).astype(jnp.int32)
    return (tokens, counts)


def draw_slot_tokens(key, part):
    return routing_draw(key)[0]


def draw_live_counts(key, part):
    return routing_draw(key)[1]


def block_scale(own_key, shape, pieces, least, top_value):
    def one(dim, blocks):
        heights = jax.random.uniform(jax.random.fold_in(jax.random.fold_in(own_key, 6), dim), (blocks,), jnp.float32, least / len(pieces), top_value / len(pieces))
        return jnp.repeat(jnp.exp(heights), shape[dim] // blocks).reshape((-1,) + (1,) * (len(shape) - dim - 1))

    loudness = one(*pieces[0])
    for cut in pieces[1:]:
        loudness = loudness * one(*cut)
    return loudness


def centred(stream_key, extent, spread, bound, cuts=(), kind=jnp.bfloat16):
    array = jax.random.normal(stream_key, extent, jnp.float32) * spread
    if len(cuts) > 0:
        array = block_scale(stream_key, extent, cuts, -0.22, 0.18) * array
    return jnp.clip(array, min=-bound, max=bound).astype(kind)


def setup_inputs(seed: int = 0) -> dict:
    key_list = jax.random.split(jax.random.key(seed), 10)
    return {
        "hidden_in": centred(key_list[0], (TOKENS, D), 1.0, 6.0, ((0, 8), (1, 4))),
        "grad_out": centred(key_list[1], (TOKENS, D), 1.0, 6.0, ((0, 8), (1, 4))),
        "slot_tokens": draw_slot_tokens(jax.random.fold_in(key_list[9], 71), 0),
        "live_counts": draw_live_counts(jax.random.fold_in(key_list[9], 71), 0),
        "norm_gain": jnp.clip(1.0 + 0.1 * jax.random.normal(key_list[4], (D,), jnp.float32), 0.5, 1.5),
        "router_weight": centred(key_list[5], (D,), D ** -0.5, 0.0625, ((0, 4),), jnp.float32),
        "gate_weight": centred(key_list[6], (D, FF), D ** -0.5, 0.0625, ((0, 4), (1, 8))),
        "up_weight": centred(key_list[7], (D, FF), D ** -0.5, 0.0625, ((0, 4), (1, 8))),
        "down_weight": centred(key_list[8], (FF, D), FF ** -0.5, 0.0390625, ((0, 8), (1, 4))),
    }


norm_eps = 1e-06

def silu_parts(gate):
    sig = jax.nn.sigmoid(gate)
    return (gate * sig, sig * (1.0 + gate * (1.0 - sig)))

def reference(hidden_in, grad_out, slot_tokens, live_counts, norm_gain, router_weight, gate_weight, up_weight, down_weight):
    slots = jnp.arange(N_SEQ * CAP, dtype=jnp.int32)
    owners = slots // CAP
    positions = (owners * TOK_DEV + slot_tokens).astype(jnp.int32)
    live_rows = slots % CAP < live_counts[owners]
    picked = jnp.take(hidden_in, positions, axis=0)
    upstream = jnp.where(live_rows[:, None], jnp.take(grad_out, positions, axis=0), jnp.zeros((), jnp.bfloat16))
    wide = picked.astype(jnp.float32)
    inverse = lax.rsqrt(lax.optimization_barrier(jnp.mean(wide * wide, axis=1, keepdims=True)) + norm_eps)
    scaled = wide * inverse
    normed = (scaled * norm_gain).astype(jnp.bfloat16)
    logits = jnp.dot(normed, router_weight.astype(jnp.bfloat16), preferred_element_type=jnp.float32)
    gate = jnp.dot(normed, gate_weight, preferred_element_type=jnp.float32)
    upper = jnp.dot(normed, up_weight, preferred_element_type=jnp.float32)
    back = jnp.dot(upstream, down_weight.T, preferred_element_type=jnp.float32)
    act, slope = silu_parts(gate)
    hidden = act * upper
    weighted = (hidden * logits[:, None]).astype(jnp.bfloat16)
    router_grad = lax.optimization_barrier(jnp.sum(hidden * back, axis=1))
    d_hidden = logits[:, None] * back
    d_gate = (d_hidden * upper * slope).astype(jnp.bfloat16)
    d_up = (d_hidden * act).astype(jnp.bfloat16)
    count_scale = lax.rsqrt(jnp.sum(live_counts).astype(jnp.float32))
    grad_gate = (count_scale * jnp.dot(normed.T, d_gate, preferred_element_type=jnp.float32)).astype(jnp.bfloat16)
    grad_up = (count_scale * jnp.dot(normed.T, d_up, preferred_element_type=jnp.float32)).astype(jnp.bfloat16)
    grad_down = (count_scale * jnp.dot(weighted.T, upstream, preferred_element_type=jnp.float32)).astype(jnp.bfloat16)
    d_normed = jnp.dot(d_gate, gate_weight.T, preferred_element_type=jnp.float32)
    d_normed = d_normed + jnp.dot(d_up, up_weight.T, preferred_element_type=jnp.float32)
    d_normed = d_normed + router_grad[:, None] * router_weight
    grad_gain = count_scale * lax.optimization_barrier(jnp.sum(d_normed * scaled, axis=0))
    grad_router = count_scale * jnp.dot(router_grad, normed.astype(jnp.float32), precision=lax.Precision.HIGHEST)
    d_scaled = d_normed * norm_gain
    d_picked = inverse * (d_scaled - scaled * lax.optimization_barrier(jnp.mean(d_scaled * scaled, axis=1, keepdims=True)))
    d_picked = jnp.where(live_rows[:, None], d_picked, jnp.zeros((), jnp.float32))
    grad_in = grad_out.astype(jnp.float32).at[positions].add(d_picked).astype(jnp.bfloat16)
    return (grad_in, grad_gate, grad_up, grad_down, grad_gain, grad_router)
```

```python
import functools

import jax
import jax.numpy as jnp
from jax import lax
from jax.experimental import pallas as pl
from jax.experimental.pallas import tpu as pltpu
from jax.sharding import PartitionSpec as P

norm_eps = 1e-06
f32 = jnp.float32
bf16 = jnp.bfloat16
MESH = pl.DeviceIdType.MESH


def pick_chunks(size, options, unit=128):
    for n in options:
        if size % (n * unit) == 0:
            return n
    return 1


def nt_dot(a, b):
    return lax.dot_general(a, b, (((1,), (1,)), ((), ())), preferred_element_type=f32)


def tn_dot(a, b):
    return lax.dot_general(a, b, (((0,), (0,)), ((), ())), preferred_element_type=f32)


def outer_kernel(
    norm, dg, du, wt, ups, hid, gout, dn, gain, sums, cs, col, tok, live, o_gate, o_up, o_down, o_in, o_gain, o_router
):
    scale = cs[0:1, 0:1]

    def fill(out, left, right):
        size = right.shape[1]
        piece = size // pick_chunks(size, (6, 4, 3, 2))
        for n in range(0, size, piece):
            out[:, n : n + piece] = (tn_dot(left, right[:, n : n + piece]) * scale).astype(bf16)

    cap = dn.shape[0]
    place = tok[...] == lax.broadcasted_iota(jnp.int32, (hid.shape[0], cap), 0)
    hot = place.astype(f32).astype(bf16)
    alive = (lax.broadcasted_iota(jnp.int32, (cap, 1), 0) < live[...]).astype(f32)
    inverse = col[0][:, 0:1]
    scaled = tn_dot(hot, hid[...]) * inverse
    d_picked = inverse * (dn[...] * gain[...] - scaled * col[1][:, 0:1]) * alive
    high = d_picked.astype(bf16)
    rest = d_picked - high.astype(f32)
    mid = rest.astype(bf16)
    low = (rest - mid.astype(f32)).astype(bf16)
    fill(o_gate, norm[...], dg)
    added = (
        jnp.dot(hot, high, preferred_element_type=f32)
        + jnp.dot(hot, mid, preferred_element_type=f32)
        + jnp.dot(hot, low, preferred_element_type=f32)
    )
    o_in[...] = (gout[...].astype(f32) + added).astype(bf16)
    o_gain[...] = sums[0:1, :] * scale
    o_router[...] = sums[1:2, :] * scale
    fill(o_up, norm[...], du)
    fill(o_down, wt[...], ups)


def outer_products(
    normed, d_gate, d_up, weighted, upstream, hid, gout, d_normed, gain, sums, cs, col, tok, live
):
    rows, width = normed.shape
    hidden = d_gate.shape[1]
    tokens, cap = hid.shape[0], d_normed.shape[0]
    steps = next(n for n in (8, 4, 2, 1) if width % (n * 128) == 0 and hidden % (n * 128) == 0)
    tw, th = width // steps, hidden // steps

    def whole(shape):
        return pl.BlockSpec(shape, lambda i: (0,) * len(shape))

    def across(height, size):
        return pl.BlockSpec((height, size), lambda i: (0, i))

    return pl.pallas_call(
        outer_kernel,
        grid=(steps,),
        out_shape=[
            jax.ShapeDtypeStruct((width, hidden), bf16),
            jax.ShapeDtypeStruct((width, hidden), bf16),
            jax.ShapeDtypeStruct((hidden, width), bf16),
            jax.ShapeDtypeStruct((tokens, width), bf16),
            jax.ShapeDtypeStruct((1, width), f32),
            jax.ShapeDtypeStruct((1, width), f32),
        ],
        in_specs=[
            across(rows, tw),
            whole((rows, hidden)),
            whole((rows, hidden)),
            across(rows, th),
            whole((rows, width)),
            across(tokens, tw),
            across(tokens, tw),
            across(cap, tw),
            across(1, tw),
            across(2, tw),
            whole(cs.shape),
            whole(col.shape),
            whole(tok.shape),
            whole(live.shape),
        ],
        out_specs=[
            pl.BlockSpec((tw, hidden), lambda i: (i, 0)),
            pl.BlockSpec((tw, hidden), lambda i: (i, 0)),
            pl.BlockSpec((th, width), lambda i: (i, 0)),
            across(tokens, tw),
            across(1, tw),
            across(1, tw),
        ],
        compiler_params=pltpu.CompilerParams(
            dimension_semantics=("arbitrary",), vmem_limit_bytes=67_043_328
        ),
    )(normed, d_gate, d_up, weighted, upstream, hid, gout, d_normed, gain, sums, cs, col, tok, live)


def kernel(
    ns,
    nt,
    nc,
    nk,
    hid,
    gout,
    tok,
    live,
    gain,
    router,
    wg_hbm,
    wu_hbm,
    wd_hbm,
    o_w,
    o_dg,
    o_du,
    o_norm,
    o_ups,
    o_gr,
    o_cs,
    o_dn,
    o_col,
    wg,
    wu,
    wd,
    own,
    qmsg,
    qrec,
    pmsg,
    prec,
    logbuf,
    rgbuf,
    rgacc,
    inacc,
    part,
    drec,
    xsnd,
    xrec,
    acc,
    ysnd,
    yrec,
    zsnd,
    zrec,
    gsnd,
    gyrec,
    gzsnd,
    gzrec,
    w_sem,
    agz_s,
    agz_r,
    agy_s,
    agy_r,
    q_s,
    q_r,
    p_s,
    p_r,
    l_s,
    l_r,
    d_s,
    d_r,
    x_s,
    x_r,
    a_s,
    a_r,
    rg_s,
    rg_r,
    y_s,
    y_r,
    z_s,
    z_r,
    gy_s,
    gy_r,
    gz_s,
    gz_r,
):
    tokens, width = hid.shape
    cap = tok.shape[1]
    rows = ns * cap
    half = rows // 2
    quarter = half // 2
    hidden = wg.shape[1]
    fc = hidden // nc
    kc = width // nk
    nz, nx = ns // 2, nt // 2
    s, t = lax.axis_index("seq"), lax.axis_index("tensor")
    y, z = lax.rem(s, 2), lax.div(s, 2)
    core, x = lax.rem(t, 2), lax.div(t, 2)
    mate = t + 1 - 2 * core
    yp = s + 1 - 2 * y
    zhalf = lax.div(z, nz // 2)
    mine = pl.multiple_of(core * half, half)

    def zx(j):
        total = 0
        bit = 1
        while bit < nz:
            b = lax.rem(lax.div(z, bit), 2)
            total = total + bit * (1 - b if j & bit else b)
            bit *= 2
        return total

    def slot_rows(yy, zz):
        return pl.ds(pl.multiple_of((yy * nz + zz) * cap, cap), cap)

    def remote(src, dst, ssem, rsem, **where):
        return pltpu.make_async_remote_copy(
            src_ref=src,
            dst_ref=dst,
            send_sem=ssem,
            recv_sem=rsem,
            device_id=where,
            device_id_type=MESH,
        )

    loads = [
        pltpu.make_async_copy(wd_hbm, wd, w_sem.at[0]),
        pltpu.make_async_copy(wg_hbm, wg, w_sem.at[1]),
        pltpu.make_async_copy(wu_hbm, wu, w_sem.at[2]),
    ]
    for load in loads:
        load.start()

    barrier = pltpu.get_barrier_semaphore()
    for j in range(1, ns):
        pl.semaphore_signal(
            barrier, inc=1, device_id={"seq": lax.rem(s + j, ns)}, device_id_type=MESH
        )
    for j in range(1, nt):
        pl.semaphore_signal(
            barrier, inc=1, device_id={"tensor": lax.rem(t + j, nt)}, device_id_type=MESH
        )

    width_total = width * nt
    place = tok[...] == lax.broadcasted_iota(jnp.int32, (tokens, cap), 0)
    hot = place.astype(f32).astype(bf16)
    alive = (lax.broadcasted_iota(jnp.int32, (cap, 1), 0) < live[...]).astype(f32)
    own_rows = slot_rows(y, z)
    o_ups[own_rows, :] = (tn_dot(hot, gout[...]) * alive).astype(bf16)
    picked = tn_dot(hot, hid[...])
    own[...] = picked
    qmsg[...] = jnp.broadcast_to(jnp.sum(picked * picked, axis=1, keepdims=True), (cap, 128))
    pl.semaphore_wait(barrier, ns - 1 + nt - 1)

    gathered = (o_ups, o_norm)

    def agz(m, j):
        block = gathered[m].at[own_rows]
        return remote(block, block, agz_s.at[m, j], agz_r.at[m, j], seq=2 * zx(j) + y)

    def agy(m, j):
        block = gathered[m].at[slot_rows(y, zx(j))]
        return remote(block, block, agy_s.at[m, j], agy_r.at[m, j], seq=yp)

    def square_copy(j):
        return remote(qmsg, qrec.at[j], q_s.at[j], q_r.at[j], tensor=lax.rem(t + j, nt))

    def spread(m):
        agy(m, 0).start()
        for j in range(1, nz):
            agz(m, j).start()

    def pass_on(m, js):
        for j in js:
            agz(m, j).wait_recv()
            agy(m, j).start()

    def arrived(m, js):
        for j in js:
            agy(m, j).wait_recv()

    for j in range(1, nt):
        square_copy(j).start()
    spread(0)
    total = qmsg[...]
    for j in range(1, nt):
        square_copy(j).wait_recv()
        total = total + qrec[j]
    inverse = lax.rsqrt(total / width_total + norm_eps)
    o_col[0] = inverse
    normed = (own[...] * inverse[:, 0:1] * gain[...]).astype(bf16)
    o_norm[own_rows, :] = normed
    router_row = router[...].astype(bf16).astype(f32)
    pmsg[...] = jnp.broadcast_to(
        jnp.sum(normed.astype(f32) * router_row, axis=1, keepdims=True), (cap, 128)
    )

    def logit_part(j):
        return remote(pmsg, prec.at[j], p_s.at[j], p_r.at[j], tensor=lax.rem(t + j, nt))

    def logit_copy(j):
        piece = logbuf.at[own_rows, :]
        return remote(piece, piece, l_s.at[j], l_r.at[j], seq=lax.rem(s + j, ns))

    def share_logits():
        total = pmsg[...]
        for j in range(1, nt):
            logit_part(j).wait_recv()
            total = total + prec[j]
        logbuf[own_rows, :] = total
        for j in range(1, ns):
            logit_copy(j).start()

    near, far = range(1, nz // 2), range(nz // 2, nz)
    for j in range(1, nt):
        logit_part(j).start()
    pass_on(0, near)
    spread(1)

    def item(i):
        if i < 2:
            h = zhalf if i == 0 else 1 - zhalf
            return 0, pl.ds(pl.multiple_of(h * quarter, quarter), quarter)
        return i - 1, pl.ds(0, half)

    def pair(i, c):
        a, span = item(i)
        return remote(
            part.at[a, c, 1 - core, span],
            drec.at[a, c, span],
            d_s.at[i, c],
            d_r.at[i, c],
            tensor=mate,
        )

    def cross(j, i, c):
        a, span = item(i)
        return remote(
            xsnd.at[a, c, span],
            xrec.at[j, a, c, span],
            x_s.at[j, i, c],
            x_r.at[j, i, c],
            tensor=2 * lax.rem(x + j, nx) + core,
        )

    def emit(i, c, value):
        a, span = item(i)
        value = value.reshape(2, -1, fc)
        part[a, c, 0, span, :] = value[0]
        part[a, c, 1, span, :] = value[1]
        pair(i, c).start()

    def relay(i, c):
        a, span = item(i)
        pair(i, c).wait_recv()
        total = part[a, c, core, span, :] + drec[a, c, span, :]
        part[a, c, core, span, :] = total
        xsnd[a, c, span, :] = total.astype(bf16)
        for j in range(1, nx):
            cross(j, i, c).start()

    def cols(c):
        return pl.ds(pl.multiple_of(c * fc, fc), fc)

    def back_pass(i, start, stop):
        _, span = item(i)
        upper_span = pl.ds(pl.multiple_of(half + span.start, quarter), quarter)

        @pl.loop(start, stop)
        def _(c):
            left = jnp.concatenate([o_ups[span, :], o_ups[upper_span, :]], axis=0)
            emit(i, c, nt_dot(left, wd[cols(c), :]))
            if i == 1 and start == 0:

                @pl.when(c == 0)
                def _():
                    relay(0, nc - 1)

            @pl.when(c > 1)
            def _():
                relay(i, c - 2)

    cut, cut2 = nc // 3, 2 * nc // 3
    loads[0].wait()
    arrived(0, [0, *near])
    back_pass(0, 0, cut)
    share_logits()
    pass_on(0, far)
    back_pass(0, cut, cut2)
    pass_on(1, near)
    back_pass(0, cut2, nc)
    relay(0, nc - 2)
    arrived(0, far)
    back_pass(1, 0, cut)
    pass_on(1, far)
    back_pass(1, cut, nc)
    relay(1, nc - 2)
    arrived(1, range(nz))
    loads[1].wait()
    loads[2].wait()

    @pl.loop(0, nc)
    def _(c):
        emit(2, c, jnp.dot(o_norm[...], wg[:, cols(c)], preferred_element_type=f32))

        @pl.when(c == 0)
        def _():
            relay(1, nc - 1)

        @pl.when(c > 0)
        def _():
            relay(2, c - 1)

        emit(3, c, jnp.dot(o_norm[...], wu[:, cols(c)], preferred_element_type=f32))

        @pl.when(c > 0)
        def _():
            relay(3, c - 1)

    relay(2, nc - 1)
    relay(3, nc - 1)

    for j in range(1, ns):
        logit_copy(j).wait_recv()
    rgacc[...] = jnp.zeros_like(rgacc)
    inacc[...] = jnp.zeros_like(inacc)
    acc[...] = jnp.zeros_like(acc)
    acts = (o_w, o_dg, o_du)

    def act_copy(a, c):
        piece = acts[a].at[pl.ds(mine, half), cols(c)]
        return remote(piece, piece, a_s.at[a, c], a_r.at[a, c], tensor=mate)

    def lanes(terms):
        add = terms[:, 0:128]
        for i in range(1, fc // 128):
            add = add + terms[:, i * 128 : (i + 1) * 128]
        return add

    def gate_backward(c):
        for i in range(4):
            for j in range(1, nx):
                cross(j, i, c).wait_recv()

        @pl.loop(0, half // 16)
        def _(r):
            sub = pl.ds(pl.multiple_of(r * 16, 16), 16)
            out = pl.ds(pl.multiple_of(mine + r * 16, 16), 16)
            back, gate, upper = [
                functools.reduce(
                    lambda u, v: u + v,
                    [xrec[j, a, c, sub, :].astype(f32) for j in range(1, nx)],
                    part[a, c, core, sub, :],
                )
                for a in range(3)
            ]
            logit = logbuf[out, 0:1]
            sig = jax.nn.sigmoid(gate)
            act = gate * sig
            slope = sig * (1.0 + gate * (1.0 - sig))
            hid_v = act * upper
            d_hidden = logit * back
            d_gate = (d_hidden * upper * slope).astype(bf16)
            d_up = (d_hidden * act).astype(bf16)
            o_w[out, cols(c)] = (hid_v * logit).astype(bf16)
            o_dg[out, cols(c)] = d_gate
            o_du[out, cols(c)] = d_up
            rgacc[sub, :] = rgacc[sub, :] + lanes(hid_v * back)
            inacc[sub, :] = inacc[sub, :] + lanes(
                d_gate.astype(f32) * gate + d_up.astype(f32) * upper
            )

        for a in range(3):
            act_copy(a, c).start()

    def kcols(k):
        return pl.ds(pl.multiple_of(k * kc, kc), kc)

    def back_dots(c, k):
        return nt_dot(o_dg[:, cols(c)], wg[kcols(k), cols(c)]) + nt_dot(
            o_du[:, cols(c)], wu[kcols(k), cols(c)]
        )

    def act_wait(c):
        for a in range(3):
            act_copy(a, c).wait_recv()

    na = nk // 2 if nk % 2 == 0 else nk
    ka = width // na

    def accumulate(c):
        act_wait(c)

        @pl.loop(0, na)
        def _(k):
            wide = pl.ds(pl.multiple_of(k * ka, ka), ka)
            total = nt_dot(o_dg[:, cols(c)], wg[wide, cols(c)]) + nt_dot(
                o_du[:, cols(c)], wu[wide, cols(c)]
            )
            acc[:, :, wide] = acc[:, :, wide] + total.reshape(ns, cap, ka)

    @pl.loop(0, nc - 1)
    def _(c):
        gate_backward(c)

        @pl.when(c > 0)
        def _():
            accumulate(c - 1)

    gate_backward(nc - 1)
    rg_half = jnp.sum(rgacc[...], axis=1, keepdims=True)
    in_half = jnp.sum(inacc[...], axis=1, keepdims=True)
    in_half = in_half + rg_half * logbuf[pl.ds(mine, half), 0:1]
    first = lax.broadcasted_iota(jnp.int32, (half, 128), 1) < 64
    rgbuf[pl.ds(mine, half), :] = jnp.where(first, rg_half, in_half)
    rg_piece = rgbuf.at[pl.ds(mine, half), :]
    rg_copy = remote(rg_piece, rg_piece, rg_s, rg_r, tensor=mate)
    rg_copy.start()
    accumulate(nc - 2)
    act_wait(nc - 1)
    rg_copy.wait_recv()

    def ycopy(k):
        return remote(ysnd.at[k], yrec.at[k], y_s.at[k], y_r.at[k], seq=yp)

    def zcopy(j, k):
        return remote(
            zsnd.at[j, k],
            zrec.at[j, k],
            z_s.at[j, k],
            z_r.at[j, k],
            seq=2 * zx(j) + y,
        )

    def zstage(k):
        ycopy(k).wait_recv()
        for j in range(1, nz):
            zz = zx(j)
            zsnd[j, k] = (acc[y * nz + zz, :, kcols(k)] + yrec[k, zz].astype(f32)).astype(bf16)
            zcopy(j, k).start()
        acc[y * nz + z, :, kcols(k)] = acc[y * nz + z, :, kcols(k)] + yrec[k, z].astype(f32)

    def finish(k):
        total = back_dots(nc - 1, k) + rgbuf[:, 0:1] * router[:, kcols(k)]
        total = acc[:, :, kcols(k)] + total.reshape(ns, cap, kc)
        acc[:, :, kcols(k)] = total
        for zz in range(nz):
            ysnd[k, zz] = acc[(1 - y) * nz + zz, :, kcols(k)].astype(bf16)
        gsnd[0:1, kcols(k)] = jnp.sum(
            total.reshape(rows, kc) * o_norm[:, kcols(k)].astype(f32), axis=0, keepdims=True
        ) / gain[:, kcols(k)]

    @pl.loop(0, nk - 1)
    def _(k):
        finish(k)
        ycopy(k).start()

    extra = gsnd.shape[1] - width
    gsnd[0:1, pl.ds(width, extra)] = rgbuf[...].T[64:65, :]
    gsnd[1:2, pl.ds(width, extra)] = jnp.broadcast_to(live[...].astype(f32), (1, extra))
    router_part = jnp.zeros((1, width), f32)
    for b in range(ns):
        block = o_norm[b * cap : (b + 1) * cap, :].astype(f32)
        router_part = router_part + jnp.sum(
            rgbuf[b * cap : (b + 1) * cap, 0:1] * block, axis=0, keepdims=True
        )
    gsnd[1:2, pl.ds(0, width)] = router_part
    finish(nk - 1)
    gy_copy = remote(gsnd, gyrec, gy_s, gy_r, seq=yp)
    gy_copy.start()
    ycopy(nk - 1).start()

    def gz_copy(j):
        return remote(gzsnd, gzrec.at[j], gz_s.at[j], gz_r.at[j], seq=2 * zx(j) + y)

    @pl.loop(0, nk - 1)
    def _(k):
        zstage(k)

    gy_copy.wait_recv()
    gzsnd[...] = gsnd[...] + gyrec[...]
    for j in range(1, nz):
        gz_copy(j).start()
    zstage(nk - 1)

    o_dn[...] = acc[y * nz + z]
    for j in range(1, nz):

        @pl.loop(0, nk)
        def _(k):
            zcopy(j, k).wait_recv()
            o_dn[:, kcols(k)] = o_dn[:, kcols(k)] + zrec[j, k].astype(f32)

    total = gzsnd[...]
    for j in range(1, nz):
        gz_copy(j).wait_recv()
        total = total + gzrec[j]
    o_gr[...] = total[:, 0:width]
    o_cs[...] = lax.rsqrt(total[1:2, width : width + 128])
    here = (y * nz + z) * cap + lax.broadcasted_iota(jnp.int32, (cap, extra), 0)
    pick = here == lax.broadcasted_iota(jnp.int32, (cap, extra), 1)
    inner = jnp.sum(jnp.where(pick, total[0:1, width:], 0.0), axis=1, keepdims=True)
    o_col[1] = jnp.broadcast_to(inner / width_total, (cap, 128))

    for m in range(2):
        agy(m, 0).wait_send()
        for j in range(1, nz):
            agz(m, j).wait_send()
            agy(m, j).wait_send()
    for j in range(1, nt):
        square_copy(j).wait_send()
        logit_part(j).wait_send()
    for j in range(1, ns):
        logit_copy(j).wait_send()
    gy_copy.wait_send()
    for j in range(1, nz):
        gz_copy(j).wait_send()
    rg_copy.wait_send()

    @pl.loop(0, nc)
    def _(c):
        for i in range(4):
            pair(i, c).wait_send()
            for j in range(1, nx):
                cross(j, i, c).wait_send()
        for a in range(3):
            act_copy(a, c).wait_send()

    @pl.loop(0, nk)
    def _(k):
        ycopy(k).wait_send()
        for j in range(1, nz):
            zcopy(j, k).wait_send()


def body(
    hidden_in,
    grad_out,
    slot_tokens,
    live_counts,
    norm_gain,
    router_weight,
    gate_weight,
    up_weight,
    down_weight,
):
    ns, nt = lax.axis_size("seq"), lax.axis_size("tensor")
    cap = slot_tokens.shape[0]
    tokens, width = hidden_in.shape
    hidden = gate_weight.shape[1]
    rows, nz, nx = ns * cap, ns // 2, nt // 2
    half = rows // 2
    nc = pick_chunks(hidden, (6, 4, 3, 2))
    nk = pick_chunks(width, (4, 2))
    fc, kc = hidden // nc, width // nk
    wide = width + rows
    vmem = pl.BlockSpec(memory_space=pltpu.VMEM)
    hbm = pl.BlockSpec(memory_space=pl.ANY)
    dma = pltpu.SemaphoreType.DMA
    tok = slot_tokens.reshape(1, cap)
    live = live_counts.reshape(1, 1)
    gain = norm_gain.reshape(1, width)
    weighted, d_gate, d_up, normed, upstream, sums, scale, d_normed, column = pl.pallas_call(
        functools.partial(kernel, ns, nt, nc, nk),
        out_shape=[
            jax.ShapeDtypeStruct((rows, hidden), bf16),
            jax.ShapeDtypeStruct((rows, hidden), bf16),
            jax.ShapeDtypeStruct((rows, hidden), bf16),
            jax.ShapeDtypeStruct((rows, width), bf16),
            jax.ShapeDtypeStruct((rows, width), bf16),
            jax.ShapeDtypeStruct((2, width), f32),
            jax.ShapeDtypeStruct((1, 128), f32),
            jax.ShapeDtypeStruct((cap, width), f32),
            jax.ShapeDtypeStruct((2, cap, 128), f32),
        ],
        in_specs=[vmem] * 6 + [hbm] * 3,
        out_specs=[vmem] * 9,
        scratch_shapes=[
            pltpu.VMEM((width, hidden), bf16),
            pltpu.VMEM((width, hidden), bf16),
            pltpu.VMEM((hidden, width), bf16),
            pltpu.VMEM((cap, width), f32),
            pltpu.VMEM((cap, 128), f32),
            pltpu.VMEM((nt, cap, 128), f32),
            pltpu.VMEM((cap, 128), f32),
            pltpu.VMEM((nt, cap, 128), f32),
            pltpu.VMEM((rows, 128), f32),
            pltpu.VMEM((rows, 128), f32),
            pltpu.VMEM((half, 128), f32),
            pltpu.VMEM((half, 128), f32),
            pltpu.VMEM((3, nc, 2, half, fc), f32),
            pltpu.VMEM((3, nc, half, fc), f32),
            pltpu.VMEM((3, nc, half, fc), bf16),
            pltpu.VMEM((nx, 3, nc, half, fc), bf16),
            pltpu.VMEM((ns, cap, width), f32),
            pltpu.VMEM((nk, nz, cap, kc), bf16),
            pltpu.VMEM((nk, nz, cap, kc), bf16),
            pltpu.VMEM((nz, nk, cap, kc), bf16),
            pltpu.VMEM((nz, nk, cap, kc), bf16),
            pltpu.VMEM((2, wide), f32),
            pltpu.VMEM((2, wide), f32),
            pltpu.VMEM((2, wide), f32),
            pltpu.VMEM((nz, 2, wide), f32),
            dma((3,)),
            dma((2, nz)),
            dma((2, nz)),
            dma((2, nz)),
            dma((2, nz)),
            dma((nt,)),
            dma((nt,)),
            dma((nt,)),
            dma((nt,)),
            dma((ns,)),
            dma((ns,)),
            dma((4, nc)),
            dma((4, nc)),
            dma((nx, 4, nc)),
            dma((nx, 4, nc)),
            dma((3, nc)),
            dma((3, nc)),
            dma,
            dma,
            dma((nk,)),
            dma((nk,)),
            dma((nz, nk)),
            dma((nz, nk)),
            dma,
            dma,
            dma((nz,)),
            dma((nz,)),
        ],
        compiler_params=pltpu.CompilerParams(
            collective_id=0, has_side_effects=True, vmem_limit_bytes=67_043_328
        ),
    )(
        hidden_in,
        grad_out,
        tok,
        live,
        gain,
        router_weight.reshape(1, width),
        gate_weight,
        up_weight,
        down_weight,
    )
    grad_gate, grad_up, grad_down, grad_in, grad_gain, grad_router = outer_products(
        normed,
        d_gate,
        d_up,
        weighted,
        upstream,
        hidden_in,
        grad_out,
        d_normed,
        gain,
        sums,
        scale,
        column,
        tok,
        live,
    )
    return (
        grad_in,
        grad_gate,
        grad_up,
        grad_down,
        grad_gain.reshape(width),
        grad_router.reshape(width),
    )


def solution(mesh):
    in_specs = (
        P("seq", "tensor"),
        P("seq", "tensor"),
        P("seq"),
        P("seq"),
        P("tensor"),
        P("tensor"),
        P("tensor", "seq"),
        P("tensor", "seq"),
        P("seq", "tensor"),
    )
    out_specs = (
        P("seq", "tensor"),
        P("tensor", "seq"),
        P("tensor", "seq"),
        P("seq", "tensor"),
        P("tensor"),
        P("tensor"),
    )
    return jax.shard_map(body, mesh=mesh, in_specs=in_specs, out_specs=out_specs, check_vma=False)
```

```python
import functools

import jax
import jax.numpy as jnp
from jax import lax
from jax.experimental import pallas as pl
from jax.experimental.pallas import tpu as pltpu
from jax.sharding import PartitionSpec as P

norm_eps = 1e-06
f32 = jnp.float32
bf16 = jnp.bfloat16
MESH = pl.DeviceIdType.MESH


def pick_chunks(size, options, unit=128):
    for n in options:
        if size % (n * unit) == 0:
            return n
    return 1


def nt_dot(a, b):
    return lax.dot_general(a, b, (((1,), (1,)), ((), ())), preferred_element_type=f32)


def tn_dot(a, b):
    return lax.dot_general(a, b, (((0,), (0,)), ((), ())), preferred_element_type=f32)


def outer_kernel(
    norm, dg, du, wt, ups, cs, tok, gout_hbm, fin_hbm, o_gate, o_up, o_down, o_in, o_gain, o_router, gout, fin, sem
):
    scale = cs[0:1, 0:1]
    step = pl.program_id(0)
    tokens = o_in.shape[0]
    cap = tok.shape[1]
    loads = [
        pltpu.make_async_copy(gout_hbm, gout, sem.at[0]),
        pltpu.make_async_copy(fin_hbm, fin, sem.at[1]),
    ]

    @pl.when(step == 0)
    def _():
        for load in loads:
            load.start()

    @pl.when(step == pl.num_programs(0) // 2)
    def _():
        for load in loads:
            load.wait()
        o_gain[...] = fin[cap : cap + 1, :]
        o_router[...] = fin[cap + 1 : cap + 2, :]
        place = tok[...] == lax.broadcasted_iota(jnp.int32, (tokens, cap), 0)
        hot = place.astype(f32).astype(bf16)
        d_picked = fin[0:cap, :]
        high = d_picked.astype(bf16)
        rest = d_picked - high.astype(f32)
        mid = rest.astype(bf16)
        low = (rest - mid.astype(f32)).astype(bf16)
        added = jnp.dot(
            jnp.concatenate([hot, hot, hot], axis=1),
            jnp.concatenate([high, mid, low], axis=0),
            preferred_element_type=f32,
        )
        o_in[...] = (gout[...].astype(f32) + added).astype(bf16)

    def fill(out, left, right):
        size = right.shape[1]
        piece = size // pick_chunks(size, (6, 4, 3, 2))
        for n in range(0, size, piece):
            out[:, n : n + piece] = (tn_dot(left, right[:, n : n + piece]) * scale).astype(bf16)

    fill(o_gate, norm[...], dg)
    fill(o_up, norm[...], du)
    fill(o_down, wt[...], ups)


def outer_products(normed, d_gate, d_up, weighted, upstream, cs, tok, gout, fin):
    rows, width = normed.shape
    hidden = d_gate.shape[1]
    tokens = gout.shape[0]
    steps = next(n for n in (8, 4, 2, 1) if width % (n * 128) == 0 and hidden % (n * 128) == 0)
    tw, th = width // steps, hidden // steps

    def whole(shape):
        return pl.BlockSpec(shape, lambda i: (0, 0))

    return pl.pallas_call(
        outer_kernel,
        grid=(steps,),
        out_shape=[
            jax.ShapeDtypeStruct((width, hidden), bf16),
            jax.ShapeDtypeStruct((width, hidden), bf16),
            jax.ShapeDtypeStruct((hidden, width), bf16),
            jax.ShapeDtypeStruct((tokens, width), bf16),
            jax.ShapeDtypeStruct((1, width), f32),
            jax.ShapeDtypeStruct((1, width), f32),
        ],
        in_specs=[
            pl.BlockSpec((rows, tw), lambda i: (0, i)),
            whole((rows, hidden)),
            whole((rows, hidden)),
            pl.BlockSpec((rows, th), lambda i: (0, i)),
            whole((rows, width)),
            whole(cs.shape),
            whole(tok.shape),
            pl.BlockSpec(memory_space=pl.ANY),
            pl.BlockSpec(memory_space=pl.ANY),
        ],
        out_specs=[
            pl.BlockSpec((tw, hidden), lambda i: (i, 0)),
            pl.BlockSpec((tw, hidden), lambda i: (i, 0)),
            pl.BlockSpec((th, width), lambda i: (i, 0)),
            whole((tokens, width)),
            whole((1, width)),
            whole((1, width)),
        ],
        scratch_shapes=[
            pltpu.VMEM(gout.shape, bf16),
            pltpu.VMEM(fin.shape, f32),
            pltpu.SemaphoreType.DMA((2,)),
        ],
        compiler_params=pltpu.CompilerParams(
            dimension_semantics=("arbitrary",), vmem_limit_bytes=67_043_328
        ),
    )(normed, d_gate, d_up, weighted, upstream, cs, tok, gout, fin)


def kernel(
    ns,
    nt,
    nc,
    nk,
    hid,
    gout,
    tok,
    live,
    gain,
    router,
    wg_hbm,
    wu_hbm,
    wd_hbm,
    h_w,
    h_dg,
    h_du,
    h_norm,
    h_ups,
    h_cs,
    h_fin,
    o_w,
    o_dg,
    o_du,
    o_norm,
    o_ups,
    o_cs,
    o_fin,
    wg,
    wu,
    wd,
    own,
    invbuf,
    qmsg,
    qrec,
    pmsg,
    prec,
    logbuf,
    rgbuf,
    rgacc,
    inacc,
    part,
    drec,
    xsnd,
    xrec,
    acc,
    ysnd,
    yrec,
    zsnd,
    zrec,
    asnd,
    ayrec,
    azsnd,
    azrec,
    bsnd,
    byrec,
    bzsnd,
    bzrec,
    w_sem,
    h_sem,
    agz_s,
    agz_r,
    agy_s,
    agy_r,
    agd_s,
    agd_r,
    q_s,
    q_r,
    p_s,
    p_r,
    l_s,
    l_r,
    d_s,
    d_r,
    x_s,
    x_r,
    a_s,
    a_r,
    rg_s,
    rg_r,
    y_s,
    y_r,
    z_s,
    z_r,
    gy_s,
    gy_r,
    gz_s,
    gz_r,
):
    tokens, width = hid.shape
    cap = tok.shape[1]
    rows = ns * cap
    half = rows // 2
    quarter = half // 2
    hidden = wg.shape[1]
    fc = hidden // nc
    kc = width // nk
    nz, nx = ns // 2, nt // 2
    s, t = lax.axis_index("seq"), lax.axis_index("tensor")
    y, z = lax.rem(s, 2), lax.div(s, 2)
    core, x = lax.rem(t, 2), lax.div(t, 2)
    mate = t + 1 - 2 * core
    yp = s + 1 - 2 * y
    zhalf = lax.div(z, nz // 2)
    mine = pl.multiple_of(core * half, half)

    def zx(j):
        total = 0
        bit = 1
        while bit < nz:
            b = lax.rem(lax.div(z, bit), 2)
            total = total + bit * (1 - b if j & bit else b)
            bit *= 2
        return total

    def slot_rows(yy, zz):
        return pl.ds(pl.multiple_of((yy * nz + zz) * cap, cap), cap)

    def remote(src, dst, ssem, rsem, **where):
        return pltpu.make_async_remote_copy(
            src_ref=src,
            dst_ref=dst,
            send_sem=ssem,
            recv_sem=rsem,
            device_id=where,
            device_id_type=MESH,
        )

    loads = [
        pltpu.make_async_copy(wd_hbm, wd, w_sem.at[0]),
        pltpu.make_async_copy(wg_hbm, wg, w_sem.at[1]),
        pltpu.make_async_copy(wu_hbm, wu, w_sem.at[2]),
    ]
    for load in loads:
        load.start()
    results = [
        pltpu.make_async_copy(o_w, h_w, h_sem.at[0]),
        pltpu.make_async_copy(o_dg, h_dg, h_sem.at[1]),
        pltpu.make_async_copy(o_du, h_du, h_sem.at[2]),
        pltpu.make_async_copy(o_norm, h_norm, h_sem.at[3]),
        pltpu.make_async_copy(o_ups, h_ups, h_sem.at[4]),
        pltpu.make_async_copy(o_cs, h_cs, h_sem.at[5]),
        pltpu.make_async_copy(o_fin, h_fin, h_sem.at[6]),
    ]

    barrier = pltpu.get_barrier_semaphore()
    for j in range(1, ns):
        pl.semaphore_signal(
            barrier, inc=1, device_id={"seq": lax.rem(s + j, ns)}, device_id_type=MESH
        )
    for j in range(1, nt):
        pl.semaphore_signal(
            barrier, inc=1, device_id={"tensor": lax.rem(t + j, nt)}, device_id_type=MESH
        )

    width_total = width * nt
    place = tok[...] == lax.broadcasted_iota(jnp.int32, (tokens, cap), 0)
    hot = place.astype(f32).astype(bf16)
    alive = (lax.broadcasted_iota(jnp.int32, (cap, 1), 0) < live[...]).astype(f32)
    own_rows = slot_rows(y, z)
    o_ups[own_rows, :] = (tn_dot(hot, gout[...]) * alive).astype(bf16)
    picked = tn_dot(hot, hid[...])
    own[...] = picked
    qmsg[...] = jnp.broadcast_to(jnp.sum(picked * picked, axis=1, keepdims=True), (cap, 128))
    pl.semaphore_wait(barrier, ns - 1 + nt - 1)

    gathered = (o_ups, o_norm)

    def agz(m, j):
        block = gathered[m].at[own_rows]
        return remote(block, block, agz_s.at[m, j], agz_r.at[m, j], seq=2 * zx(j) + y)

    near, far = range(1, nz // 2), range(nz // 2)
    nzh = nz // 2
    rank = (1 - zhalf) * (nzh - 1 - z) + zhalf * (z - nzh)

    def far_z(f):
        return zhalf * (nzh - 1 - f) + (1 - zhalf) * (nzh + f)

    def agf(m, f):
        block = gathered[m].at[own_rows]
        return remote(
            block, block, agz_s.at[m, nzh + f], agz_r.at[m, nzh + rank], seq=2 * far_z(f) + y
        )

    def agf_in(m, f):
        block = gathered[m].at[slot_rows(y, far_z(f))]
        return remote(
            block, block, agz_s.at[m, nzh + f], agz_r.at[m, nzh + f], seq=2 * far_z(f) + y
        )

    def agy_own(m):
        block = gathered[m].at[own_rows]
        return remote(block, block, agy_s.at[m, 0], agy_r.at[m, 0], seq=yp)

    def agy(m, f):
        block = gathered[m].at[slot_rows(y, far_z(f))]
        return remote(block, block, agy_s.at[m, nzh + f], agy_r.at[m, nzh + f], seq=yp)

    def agd(m, j):
        block = gathered[m].at[own_rows]
        return remote(block, block, agd_s.at[m, j], agd_r.at[m, j], seq=2 * zx(j) + 1 - y)

    def square_copy(j):
        return remote(qmsg, qrec.at[j], q_s.at[j], q_r.at[j], tensor=lax.rem(t + j, nt))

    def spread_near(m):
        agy_own(m).start()
        for j in near:
            agz(m, j).start()
            agd(m, j).start()

    def spread_far(m, fs):
        for f in fs:
            agf(m, f).start()

    def pass_on(m, fs):
        for f in fs:
            agf_in(m, f).wait_recv()
            agy(m, f).start()

    def arrived_near(m):
        agy_own(m).wait_recv()
        for j in near:
            agz(m, j).wait_recv()
            agd(m, j).wait_recv()

    def arrived_far(m):
        for j in far:
            agy(m, j).wait_recv()

    for j in range(1, nt):
        square_copy(j).start()
    spread_near(0)
    spread_far(0, far[:1])
    total = qmsg[...]
    for j in range(1, nt):
        square_copy(j).wait_recv()
        total = total + qrec[j]
    spread_far(0, far[1:])
    inverse = lax.rsqrt(total / width_total + norm_eps)
    invbuf[...] = inverse
    normed = (own[...] * inverse[:, 0:1] * gain[...]).astype(bf16)
    o_norm[own_rows, :] = normed
    router_row = router[...].astype(bf16).astype(f32)
    pmsg[...] = jnp.broadcast_to(
        jnp.sum(normed.astype(f32) * router_row, axis=1, keepdims=True), (cap, 128)
    )

    def logit_part(j):
        return remote(pmsg, prec.at[j], p_s.at[j], p_r.at[j], tensor=lax.rem(t + j, nt))

    def logit_copy(j):
        piece = logbuf.at[own_rows, :]
        return remote(piece, piece, l_s.at[j], l_r.at[j], seq=lax.rem(s + j, ns))

    def share_logits():
        total = pmsg[...]
        for j in range(1, nt):
            logit_part(j).wait_recv()
            total = total + prec[j]
        logbuf[own_rows, :] = total
        for j in range(1, ns):
            logit_copy(j).start()

    spread_near(1)
    spread_far(1, far)
    for j in range(1, nt):
        logit_part(j).start()

    def item(i):
        if i == 4:
            return 2, pl.ds(0, half)
        h = 1 - zhalf if i % 2 else zhalf
        return i // 2, pl.ds(pl.multiple_of(h * quarter, quarter), quarter)

    def pair(i, c):
        a, span = item(i)
        return remote(
            part.at[a, c, 1 - core, span],
            drec.at[a, c, span],
            d_s.at[i, c],
            d_r.at[i, c],
            tensor=mate,
        )

    def cross(j, i, c):
        a, span = item(i)
        return remote(
            xsnd.at[a, c, span],
            xrec.at[j, a, c, span],
            x_s.at[j, i, c],
            x_r.at[j, i, c],
            tensor=2 * lax.rem(x + j, nx) + core,
        )

    def emit(i, c, value):
        a, span = item(i)
        value = value.reshape(2, -1, fc)
        part[a, c, 0, span, :] = value[0]
        part[a, c, 1, span, :] = value[1]
        pair(i, c).start()

    def relay(i, c):
        a, span = item(i)
        pair(i, c).wait_recv()
        total = part[a, c, core, span, :] + drec[a, c, span, :]
        part[a, c, core, span, :] = total
        xsnd[a, c, span, :] = total.astype(bf16)
        for j in range(1, nx):
            cross(j, i, c).start()

    def cols(c):
        return pl.ds(pl.multiple_of(c * fc, fc), fc)

    def product(i, c):
        if i == 4:
            return jnp.dot(o_norm[...], wu[:, cols(c)], preferred_element_type=f32)
        span = item(i)[1]
        span_b = pl.ds(pl.multiple_of(half + span.start, quarter), quarter)
        rows_of = gathered[i // 2]
        left = jnp.concatenate([rows_of[span, :], rows_of[span_b, :]], axis=0)
        if i < 2:
            return nt_dot(left, wd[cols(c), :])
        return jnp.dot(left, wg[:, cols(c)], preferred_element_type=f32)

    def row_pass(i, start, stop, lag, before=()):
        @pl.loop(start, stop)
        def _(c):
            emit(i, c, product(i, c))
            if before:

                @pl.when(c == 0)
                def _():
                    for b in before:
                        relay(*b)

            @pl.when(c >= lag)
            def _():
                relay(i, c - lag)

    cut, cut2 = nc // 3, 2 * nc // 3
    far_a, far_b = far[: len(far) // 2], far[len(far) // 2 :]
    loads[0].wait()
    arrived_near(0)
    row_pass(0, 0, cut, 2)
    share_logits()
    row_pass(0, cut, cut2, 2)
    pass_on(0, far_a)
    row_pass(0, cut2, nc, 2)
    relay(0, nc - 2)
    pass_on(0, far_b)
    loads[1].wait()
    arrived_near(1)
    row_pass(2, 0, cut2, 3, [(0, nc - 1)])
    pass_on(1, far_a)
    row_pass(2, cut2, nc, 3)
    relay(2, nc - 3)
    arrived_far(0)
    results[4].start()
    row_pass(1, 0, cut, 2, [(2, nc - 2), (2, nc - 1)])
    pass_on(1, far_b)
    row_pass(1, cut, nc, 2)
    relay(1, nc - 2)
    loads[2].wait()
    arrived_far(1)
    results[3].start()

    @pl.loop(0, nc)
    def _(c):
        values = [product(3, c), product(4, c)]
        emit(3, c, values[0])
        emit(4, c, values[1])

        @pl.when(c == 0)
        def _():
            relay(1, nc - 1)

        @pl.when(c > 0)
        def _():
            relay(3, c - 1)
            relay(4, c - 1)

    relay(3, nc - 1)
    relay(4, nc - 1)
    for j in range(1, ns):
        logit_copy(j).wait_recv()
    rgacc[...] = jnp.zeros_like(rgacc)
    inacc[...] = jnp.zeros_like(inacc)
    acc[...] = jnp.zeros_like(acc)
    acts = (o_w, o_dg, o_du)

    def act_copy(a, c):
        piece = acts[a].at[pl.ds(mine, half), cols(c)]
        return remote(piece, piece, a_s.at[a, c], a_r.at[a, c], tensor=mate)

    def lanes(terms):
        add = terms[:, 0:128]
        for i in range(1, fc // 128):
            add = add + terms[:, i * 128 : (i + 1) * 128]
        return add

    def gate_backward(c):
        for i in range(5):
            for j in range(1, nx):
                cross(j, i, c).wait_recv()

        @pl.loop(0, half // 16)
        def _(r):
            sub = pl.ds(pl.multiple_of(r * 16, 16), 16)
            out = pl.ds(pl.multiple_of(mine + r * 16, 16), 16)
            back, gate, upper = [
                functools.reduce(
                    lambda u, v: u + v,
                    [xrec[j, a, c, sub, :].astype(f32) for j in range(1, nx)],
                    part[a, c, core, sub, :],
                )
                for a in range(3)
            ]
            logit = logbuf[out, 0:1]
            sig = jax.nn.sigmoid(gate)
            act = gate * sig
            slope = sig * (1.0 + gate * (1.0 - sig))
            hid_v = act * upper
            d_hidden = logit * back
            d_gate = (d_hidden * upper * slope).astype(bf16)
            d_up = (d_hidden * act).astype(bf16)
            o_w[out, cols(c)] = (hid_v * logit).astype(bf16)
            o_dg[out, cols(c)] = d_gate
            o_du[out, cols(c)] = d_up
            rgacc[sub, :] = rgacc[sub, :] + lanes(hid_v * back)
            inacc[sub, :] = inacc[sub, :] + lanes(
                d_gate.astype(f32) * gate + d_up.astype(f32) * upper
            )

        for a in range(3):
            act_copy(a, c).start()

    def kcols(k):
        return pl.ds(pl.multiple_of(k * kc, kc), kc)

    def back_dots(c, k):
        return nt_dot(o_dg[:, cols(c)], wg[kcols(k), cols(c)]) + nt_dot(
            o_du[:, cols(c)], wu[kcols(k), cols(c)]
        )

    def act_wait(c):
        for a in range(3):
            act_copy(a, c).wait_recv()

    def accumulate(c, start, stop):
        wide = pl.ds(start, stop - start)
        total = nt_dot(o_dg[:, cols(c)], wg[wide, cols(c)]) + nt_dot(
            o_du[:, cols(c)], wu[wide, cols(c)]
        )
        acc[:, :, wide] = acc[:, :, wide] + total.reshape(ns, cap, stop - start)

    @pl.loop(0, nc - 1)
    def _(c):
        gate_backward(c)

        @pl.when(c > 0)
        def _():
            act_wait(c - 1)
            accumulate(c - 1, 0, width // 2)
            accumulate(c - 1, width // 2, width)

    gate_backward(nc - 1)
    split = nk // 2
    rg_half = jnp.sum(rgacc[...], axis=1, keepdims=True)
    in_half = jnp.sum(inacc[...], axis=1, keepdims=True)
    in_half = in_half + rg_half * logbuf[pl.ds(mine, half), 0:1]
    first = lax.broadcasted_iota(jnp.int32, (half, 128), 1) < 64
    rgbuf[pl.ds(mine, half), :] = jnp.where(first, rg_half, in_half)
    rg_piece = rgbuf.at[pl.ds(mine, half), :]
    rg_copy = remote(rg_piece, rg_piece, rg_s, rg_r, tensor=mate)
    rg_copy.start()
    act_wait(nc - 2)
    accumulate(nc - 2, 0, split * kc)
    act_wait(nc - 1)
    for a in range(3):
        results[a].start()
    rg_copy.wait_recv()

    def ycopy(k):
        return remote(ysnd.at[k], yrec.at[k], y_s.at[k], y_r.at[k], seq=yp)

    def zcopy(j, k):
        return remote(
            zsnd.at[j, k],
            zrec.at[j, k],
            z_s.at[j, k],
            z_r.at[j, k],
            seq=2 * zx(j) + y,
        )

    def zstage(k):
        ycopy(k).wait_recv()
        for j in range(1, nz):
            zz = zx(j)
            zsnd[j, k] = (acc[y * nz + zz, :, kcols(k)] + yrec[k, zz].astype(f32)).astype(bf16)
            zcopy(j, k).start()
        acc[y * nz + z, :, kcols(k)] = acc[y * nz + z, :, kcols(k)] + yrec[k, z].astype(f32)

    def finish(k):
        total = back_dots(nc - 1, k) + rgbuf[:, 0:1] * router[:, kcols(k)]
        total = acc[:, :, kcols(k)] + total.reshape(ns, cap, kc)
        acc[:, :, kcols(k)] = total
        for zz in range(nz):
            ysnd[k, zz] = acc[(1 - y) * nz + zz, :, kcols(k)].astype(bf16)
        bsnd[:, kcols(k)] = jnp.sum(
            total.reshape(rows, kc) * o_norm[:, kcols(k)].astype(f32), axis=0, keepdims=True
        ) / gain[:, kcols(k)]

    def sum_y(i):
        return remote(sums[i][0], sums[i][1], gy_s.at[i], gy_r.at[i], seq=yp)

    def sum_z(i, j):
        return remote(
            sums[i][2], sums[i][3].at[j], gz_s.at[i, j], gz_r.at[i, j], seq=2 * zx(j) + y
        )

    def sum_middle(i):
        sum_y(i).wait_recv()
        sums[i][2][...] = sums[i][0][...] + sums[i][1][...]
        for j in range(1, nz):
            sum_z(i, j).start()

    def sum_end(i):
        total = sums[i][2][...]
        for j in range(1, nz):
            sum_z(i, j).wait_recv()
            total = total + sums[i][3][j]
        return total

    sums = ((asnd, ayrec, azsnd, azrec), (bsnd, byrec, bzsnd, bzrec))
    finish(0)
    ycopy(0).start()
    router_part = jnp.zeros((1, width), f32)
    for b in range(ns):
        block = o_norm[b * cap : (b + 1) * cap, :].astype(f32)
        router_part = router_part + jnp.sum(
            rgbuf[b * cap : (b + 1) * cap, 0:1] * block, axis=0, keepdims=True
        )
    asnd[:, pl.ds(0, width)] = router_part
    asnd[:, pl.ds(width, rows)] = rgbuf[...].T[64:65, :]
    asnd[:, pl.ds(width + rows, 128)] = jnp.broadcast_to(live[...].astype(f32), (1, 128))
    sum_y(0).start()
    held = max(nk - 2, 1)

    @pl.loop(1, split)
    def _(k):
        finish(k)
        ycopy(k).start()

    accumulate(nc - 2, split * kc, width)

    @pl.loop(split, held)
    def _(k):
        finish(k)
        ycopy(k).start()

    for k in range(held, nk):
        finish(k)
    sum_y(1).start()
    for k in range(held, nk):
        ycopy(k).start()
    zstage(0)
    sum_middle(0)

    @pl.loop(1, held)
    def _(k):
        zstage(k)

    sum_middle(1)
    for k in range(held, nk):
        zstage(k)
    total = sum_end(0)
    scale = lax.rsqrt(total[:, width + rows :])
    o_cs[...] = scale
    results[5].start()
    o_fin[cap : cap + 8, :] = jnp.zeros((8, width), f32)
    o_fin[cap + 1 : cap + 2, :] = total[:, 0:width] * scale[:, 0:1]
    here = (y * nz + z) * cap + lax.broadcasted_iota(jnp.int32, (cap, rows), 0)
    pick = here == lax.broadcasted_iota(jnp.int32, (cap, rows), 1)
    inner = jnp.sum(
        jnp.where(pick, total[:, width : width + rows], 0.0), axis=1, keepdims=True
    )
    inner = inner / width_total
    inverse = invbuf[:, 0:1]
    alive = (lax.broadcasted_iota(jnp.int32, (cap, 1), 0) < live[...]).astype(f32)
    o_fin[cap : cap + 1, :] = sum_end(1) * scale[:, 0:1]

    @pl.loop(0, nk)
    def _(k):
        d_normed = acc[y * nz + z, :, kcols(k)]
        for j in range(1, nz):
            zcopy(j, k).wait_recv()
            d_normed = d_normed + zrec[j, k].astype(f32)
        scaled = own[:, kcols(k)] * inverse
        o_fin[0:cap, kcols(k)] = (
            inverse * (d_normed * gain[:, kcols(k)] - scaled * inner) * alive
        )

    results[6].start()
    for m in range(2):
        agy_own(m).wait_send()
        for j in near:
            agz(m, j).wait_send()
            agd(m, j).wait_send()
        for j in far:
            agf(m, j).wait_send()
            agy(m, j).wait_send()
    for j in range(1, nt):
        square_copy(j).wait_send()
        logit_part(j).wait_send()
    for j in range(1, ns):
        logit_copy(j).wait_send()
    for i in range(2):
        sum_y(i).wait_send()
        for j in range(1, nz):
            sum_z(i, j).wait_send()
    rg_copy.wait_send()

    @pl.loop(0, nc)
    def _(c):
        for i in range(5):
            pair(i, c).wait_send()
            for j in range(1, nx):
                cross(j, i, c).wait_send()
        for a in range(3):
            act_copy(a, c).wait_send()

    @pl.loop(0, nk)
    def _(k):
        ycopy(k).wait_send()
        for j in range(1, nz):
            zcopy(j, k).wait_send()

    for result in results:
        result.wait()


def body(
    hidden_in,
    grad_out,
    slot_tokens,
    live_counts,
    norm_gain,
    router_weight,
    gate_weight,
    up_weight,
    down_weight,
):
    ns, nt = lax.axis_size("seq"), lax.axis_size("tensor")
    cap = slot_tokens.shape[0]
    tokens, width = hidden_in.shape
    hidden = gate_weight.shape[1]
    rows, nz, nx = ns * cap, ns // 2, nt // 2
    half = rows // 2
    nc = pick_chunks(hidden, (6, 4, 3, 2))
    nk = pick_chunks(width, (8, 4, 2))
    fc, kc = hidden // nc, width // nk
    wide = width + rows + 128
    vmem = pl.BlockSpec(memory_space=pltpu.VMEM)
    hbm = pl.BlockSpec(memory_space=pl.ANY)
    dma = pltpu.SemaphoreType.DMA
    tok = slot_tokens.reshape(1, cap)
    live = live_counts.reshape(1, 1)
    gain = norm_gain.reshape(1, width)
    weighted, d_gate, d_up, normed, upstream, scale, final = pl.pallas_call(
        functools.partial(kernel, ns, nt, nc, nk),
        out_shape=[
            jax.ShapeDtypeStruct((rows, hidden), bf16),
            jax.ShapeDtypeStruct((rows, hidden), bf16),
            jax.ShapeDtypeStruct((rows, hidden), bf16),
            jax.ShapeDtypeStruct((rows, width), bf16),
            jax.ShapeDtypeStruct((rows, width), bf16),
            jax.ShapeDtypeStruct((1, 128), f32),
            jax.ShapeDtypeStruct((cap + 8, width), f32),
        ],
        in_specs=[vmem] * 6 + [hbm] * 3,
        out_specs=[hbm] * 7,
        scratch_shapes=[
            pltpu.VMEM((rows, hidden), bf16),
            pltpu.VMEM((rows, hidden), bf16),
            pltpu.VMEM((rows, hidden), bf16),
            pltpu.VMEM((rows, width), bf16),
            pltpu.VMEM((rows, width), bf16),
            pltpu.VMEM((1, 128), f32),
            pltpu.VMEM((cap + 8, width), f32),
            pltpu.VMEM((width, hidden), bf16),
            pltpu.VMEM((width, hidden), bf16),
            pltpu.VMEM((hidden, width), bf16),
            pltpu.VMEM((cap, width), f32),
            pltpu.VMEM((cap, 128), f32),
            pltpu.VMEM((cap, 128), f32),
            pltpu.VMEM((nt, cap, 128), f32),
            pltpu.VMEM((cap, 128), f32),
            pltpu.VMEM((nt, cap, 128), f32),
            pltpu.VMEM((rows, 128), f32),
            pltpu.VMEM((rows, 128), f32),
            pltpu.VMEM((half, 128), f32),
            pltpu.VMEM((half, 128), f32),
            pltpu.VMEM((3, nc, 2, half, fc), f32),
            pltpu.VMEM((3, nc, half, fc), f32),
            pltpu.VMEM((3, nc, half, fc), bf16),
            pltpu.VMEM((nx, 3, nc, half, fc), bf16),
            pltpu.VMEM((ns, cap, width), f32),
            pltpu.VMEM((nk, nz, cap, kc), bf16),
            pltpu.VMEM((nk, nz, cap, kc), bf16),
            pltpu.VMEM((nz, nk, cap, kc), bf16),
            pltpu.VMEM((nz, nk, cap, kc), bf16),
            pltpu.VMEM((1, wide), f32),
            pltpu.VMEM((1, wide), f32),
            pltpu.VMEM((1, wide), f32),
            pltpu.VMEM((nz, 1, wide), f32),
            pltpu.VMEM((1, width), f32),
            pltpu.VMEM((1, width), f32),
            pltpu.VMEM((1, width), f32),
            pltpu.VMEM((nz, 1, width), f32),
            dma((3,)),
            dma((7,)),
            dma((2, nz)),
            dma((2, nz)),
            dma((2, nz)),
            dma((2, nz)),
            dma((2, nz)),
            dma((2, nz)),
            dma((nt,)),
            dma((nt,)),
            dma((nt,)),
            dma((nt,)),
            dma((ns,)),
            dma((ns,)),
            dma((5, nc)),
            dma((5, nc)),
            dma((nx, 5, nc)),
            dma((nx, 5, nc)),
            dma((3, nc)),
            dma((3, nc)),
            dma,
            dma,
            dma((nk,)),
            dma((nk,)),
            dma((nz, nk)),
            dma((nz, nk)),
            dma((2,)),
            dma((2,)),
            dma((2, nz)),
            dma((2, nz)),
        ],
        compiler_params=pltpu.CompilerParams(
            collective_id=0, has_side_effects=True, vmem_limit_bytes=67_043_328
        ),
    )(
        hidden_in,
        grad_out,
        tok,
        live,
        gain,
        router_weight.reshape(1, width),
        gate_weight,
        up_weight,
        down_weight,
    )
    grad_gate, grad_up, grad_down, grad_in, grad_gain, grad_router = outer_products(
        normed,
        d_gate,
        d_up,
        weighted,
        upstream,
        scale,
        tok,
        grad_out,
        final,
    )
    return (
        grad_in,
        grad_gate,
        grad_up,
        grad_down,
        grad_gain.reshape(width),
        grad_router.reshape(width),
    )


def solution(mesh):
    in_specs = (
        P("seq", "tensor"),
        P("seq", "tensor"),
        P("seq"),
        P("seq"),
        P("tensor"),
        P("tensor"),
        P("tensor", "seq"),
        P("tensor", "seq"),
        P("seq", "tensor"),
    )
    out_specs = (
        P("seq", "tensor"),
        P("tensor", "seq"),
        P("tensor", "seq"),
        P("seq", "tensor"),
        P("tensor"),
        P("tensor"),
    )
    return jax.shard_map(body, mesh=mesh, in_specs=in_specs, out_specs=out_specs, check_vma=False)
```

```python
import functools

import jax
import jax.numpy as jnp
from jax import lax
from jax.experimental import pallas as pl
from jax.experimental.pallas import tpu as pltpu
from jax.sharding import PartitionSpec as P

norm_eps = 1e-06
f32 = jnp.float32
bf16 = jnp.bfloat16
MESH = pl.DeviceIdType.MESH


def pick_chunks(size, options, unit=128):
    for n in options:
        if size % (n * unit) == 0:
            return n
    return 1


def nt_dot(a, b):
    return lax.dot_general(a, b, (((1,), (1,)), ((), ())), preferred_element_type=f32)


def tn_dot(a, b):
    return lax.dot_general(a, b, (((0,), (0,)), ((), ())), preferred_element_type=f32)


def outer_kernel(
    norm, dg, du, wt, ups, cs, tok, gout_hbm, fin_hbm, o_gate, o_up, o_down, o_in, o_gain, o_router, gout, fin, sem
):
    scale = cs[0:1, 0:1]
    step = pl.program_id(0)
    tokens = o_in.shape[0]
    cap = tok.shape[1]
    loads = [
        pltpu.make_async_copy(gout_hbm, gout, sem.at[0]),
        pltpu.make_async_copy(fin_hbm, fin, sem.at[1]),
    ]

    @pl.when(step == 0)
    def _():
        for load in loads:
            load.start()

    @pl.when(step == pl.num_programs(0) // 2)
    def _():
        for load in loads:
            load.wait()
        o_gain[...] = fin[cap : cap + 1, :]
        o_router[...] = fin[cap + 1 : cap + 2, :]
        place = tok[...] == lax.broadcasted_iota(jnp.int32, (tokens, cap), 0)
        hot = place.astype(f32).astype(bf16)
        d_picked = fin[0:cap, :]
        high = d_picked.astype(bf16)
        rest = d_picked - high.astype(f32)
        mid = rest.astype(bf16)
        low = (rest - mid.astype(f32)).astype(bf16)
        added = jnp.dot(
            jnp.concatenate([hot, hot, hot], axis=1),
            jnp.concatenate([high, mid, low], axis=0),
            preferred_element_type=f32,
        )
        o_in[...] = (gout[...].astype(f32) + added).astype(bf16)

    def fill(out, left, right):
        size = right.shape[1]
        piece = size // pick_chunks(size, (6, 4, 3, 2))
        for n in range(0, size, piece):
            out[:, n : n + piece] = (tn_dot(left, right[:, n : n + piece]) * scale).astype(bf16)

    fill(o_gate, norm[...], dg)
    fill(o_up, norm[...], du)
    fill(o_down, wt[...], ups)


def outer_products(normed, d_gate, d_up, weighted, upstream, cs, tok, gout, fin):
    rows, width = normed.shape
    hidden = d_gate.shape[1]
    tokens = gout.shape[0]
    steps = next(n for n in (8, 4, 2, 1) if width % (n * 128) == 0 and hidden % (n * 128) == 0)
    tw, th = width // steps, hidden // steps

    def whole(shape):
        return pl.BlockSpec(shape, lambda i: (0, 0))

    return pl.pallas_call(
        outer_kernel,
        grid=(steps,),
        out_shape=[
            jax.ShapeDtypeStruct((width, hidden), bf16),
            jax.ShapeDtypeStruct((width, hidden), bf16),
            jax.ShapeDtypeStruct((hidden, width), bf16),
            jax.ShapeDtypeStruct((tokens, width), bf16),
            jax.ShapeDtypeStruct((1, width), f32),
            jax.ShapeDtypeStruct((1, width), f32),
        ],
        in_specs=[
            pl.BlockSpec((rows, tw), lambda i: (0, i)),
            whole((rows, hidden)),
            whole((rows, hidden)),
            pl.BlockSpec((rows, th), lambda i: (0, i)),
            whole((rows, width)),
            whole(cs.shape),
            whole(tok.shape),
            pl.BlockSpec(memory_space=pl.ANY),
            pl.BlockSpec(memory_space=pl.ANY),
        ],
        out_specs=[
            pl.BlockSpec((tw, hidden), lambda i: (i, 0)),
            pl.BlockSpec((tw, hidden), lambda i: (i, 0)),
            pl.BlockSpec((th, width), lambda i: (i, 0)),
            whole((tokens, width)),
            whole((1, width)),
            whole((1, width)),
        ],
        scratch_shapes=[
            pltpu.VMEM(gout.shape, bf16),
            pltpu.VMEM(fin.shape, f32),
            pltpu.SemaphoreType.DMA((2,)),
        ],
        compiler_params=pltpu.CompilerParams(
            dimension_semantics=("arbitrary",), vmem_limit_bytes=67_043_328
        ),
    )(normed, d_gate, d_up, weighted, upstream, cs, tok, gout, fin)


def kernel(
    ns,
    nt,
    nc,
    nk,
    hid,
    gout,
    tok,
    live,
    gain,
    router,
    wg_hbm,
    wu_hbm,
    wd_hbm,
    h_w,
    h_dg,
    h_du,
    h_norm,
    h_ups,
    h_cs,
    h_fin,
    o_w,
    o_dg,
    o_du,
    o_norm,
    o_ups,
    o_cs,
    o_fin,
    wg,
    wu,
    wd,
    own,
    invbuf,
    qmsg,
    qrec,
    pmsg,
    prec,
    logbuf,
    rgbuf,
    rgacc,
    inacc,
    part,
    drec,
    xsnd,
    xrec,
    acc,
    ysnd,
    yrec,
    zsnd,
    zrec,
    asnd,
    ayrec,
    azsnd,
    azrec,
    bsnd,
    byrec,
    bzsnd,
    bzrec,
    w_sem,
    h_sem,
    agz_s,
    agz_r,
    agy_s,
    agy_r,
    agd_s,
    agd_r,
    q_s,
    q_r,
    p_s,
    p_r,
    l_s,
    l_r,
    d_s,
    d_r,
    x_s,
    x_r,
    a_s,
    a_r,
    rg_s,
    rg_r,
    y_s,
    y_r,
    z_s,
    z_r,
    gy_s,
    gy_r,
    gz_s,
    gz_r,
):
    tokens, width = hid.shape
    cap = tok.shape[1]
    rows = ns * cap
    half = rows // 2
    quarter = half // 2
    hidden = wg.shape[1]
    fc = hidden // nc
    kc = width // nk
    nz, nx = ns // 2, nt // 2
    s, t = lax.axis_index("seq"), lax.axis_index("tensor")
    y, z = lax.rem(s, 2), lax.div(s, 2)
    core, x = lax.rem(t, 2), lax.div(t, 2)
    mate = t + 1 - 2 * core
    yp = s + 1 - 2 * y
    zhalf = lax.div(z, nz // 2)
    mine = pl.multiple_of(core * half, half)

    def zx(j):
        total = 0
        bit = 1
        while bit < nz:
            b = lax.rem(lax.div(z, bit), 2)
            total = total + bit * (1 - b if j & bit else b)
            bit *= 2
        return total

    def slot_rows(yy, zz):
        return pl.ds(pl.multiple_of((yy * nz + zz) * cap, cap), cap)

    def remote(src, dst, ssem, rsem, **where):
        return pltpu.make_async_remote_copy(
            src_ref=src,
            dst_ref=dst,
            send_sem=ssem,
            recv_sem=rsem,
            device_id=where,
            device_id_type=MESH,
        )

    loads = [
        pltpu.make_async_copy(wd_hbm, wd, w_sem.at[0]),
        pltpu.make_async_copy(wg_hbm, wg, w_sem.at[1]),
        pltpu.make_async_copy(wu_hbm, wu, w_sem.at[2]),
    ]
    for load in loads:
        load.start()
    results = [
        pltpu.make_async_copy(o_w, h_w, h_sem.at[0]),
        pltpu.make_async_copy(o_dg, h_dg, h_sem.at[1]),
        pltpu.make_async_copy(o_du, h_du, h_sem.at[2]),
        pltpu.make_async_copy(o_norm, h_norm, h_sem.at[3]),
        pltpu.make_async_copy(o_ups, h_ups, h_sem.at[4]),
        pltpu.make_async_copy(o_cs, h_cs, h_sem.at[5]),
        pltpu.make_async_copy(o_fin, h_fin, h_sem.at[6]),
    ]

    barrier = pltpu.get_barrier_semaphore()
    for j in range(1, ns):
        pl.semaphore_signal(
            barrier, inc=1, device_id={"seq": lax.rem(s + j, ns)}, device_id_type=MESH
        )
    for j in range(1, nt):
        pl.semaphore_signal(
            barrier, inc=1, device_id={"tensor": lax.rem(t + j, nt)}, device_id_type=MESH
        )

    width_total = width * nt
    place = tok[...] == lax.broadcasted_iota(jnp.int32, (tokens, cap), 0)
    hot = place.astype(f32).astype(bf16)
    alive = (lax.broadcasted_iota(jnp.int32, (cap, 1), 0) < live[...]).astype(f32)
    own_rows = slot_rows(y, z)
    o_ups[own_rows, :] = (tn_dot(hot, gout[...]) * alive).astype(bf16)
    picked = tn_dot(hot, hid[...])
    own[...] = picked
    qmsg[...] = jnp.broadcast_to(jnp.sum(picked * picked, axis=1, keepdims=True), (cap, 128))
    pl.semaphore_wait(barrier, ns - 1 + nt - 1)

    gathered = (o_ups, o_norm)

    def agz(m, j):
        block = gathered[m].at[own_rows]
        return remote(block, block, agz_s.at[m, j], agz_r.at[m, j], seq=2 * zx(j) + y)

    near, far = range(1, nz // 2), range(nz // 2)
    nzh = nz // 2
    rank = (1 - zhalf) * (nzh - 1 - z) + zhalf * (z - nzh)

    def far_z(f):
        return zhalf * (nzh - 1 - f) + (1 - zhalf) * (nzh + f)

    def agf(m, f):
        block = gathered[m].at[own_rows]
        return remote(
            block, block, agz_s.at[m, nzh + f], agz_r.at[m, nzh + rank], seq=2 * far_z(f) + y
        )

    def agf_in(m, f):
        block = gathered[m].at[slot_rows(y, far_z(f))]
        return remote(
            block, block, agz_s.at[m, nzh + f], agz_r.at[m, nzh + f], seq=2 * far_z(f) + y
        )

    def agy_own(m):
        block = gathered[m].at[own_rows]
        return remote(block, block, agy_s.at[m, 0], agy_r.at[m, 0], seq=yp)

    def agy(m, f):
        block = gathered[m].at[slot_rows(y, far_z(f))]
        return remote(block, block, agy_s.at[m, nzh + f], agy_r.at[m, nzh + f], seq=yp)

    def agd(m, j):
        block = gathered[m].at[own_rows]
        return remote(block, block, agd_s.at[m, j], agd_r.at[m, j], seq=2 * zx(j) + 1 - y)

    def square_copy(j):
        return remote(qmsg, qrec.at[j], q_s.at[j], q_r.at[j], tensor=lax.rem(t + j, nt))

    def spread_near(m):
        agy_own(m).start()
        for j in near:
            agz(m, j).start()
            agd(m, j).start()

    def spread_far(m, fs):
        for f in fs:
            agf(m, f).start()

    def pass_on(m, fs):
        for f in fs:
            agf_in(m, f).wait_recv()
            agy(m, f).start()

    def arrived_near(m):
        agy_own(m).wait_recv()
        for j in near:
            agz(m, j).wait_recv()
            agd(m, j).wait_recv()

    def arrived_far(m):
        for j in far:
            agy(m, j).wait_recv()

    for j in range(1, nt):
        square_copy(j).start()
    spread_near(0)
    spread_far(0, far[:1])
    total = qmsg[...]
    for j in range(1, nt):
        square_copy(j).wait_recv()
        total = total + qrec[j]
    spread_far(0, far[1:])
    inverse = lax.rsqrt(total / width_total + norm_eps)
    invbuf[...] = inverse
    normed = (own[...] * inverse[:, 0:1] * gain[...]).astype(bf16)
    o_norm[own_rows, :] = normed
    router_row = router[...].astype(bf16).astype(f32)
    pmsg[...] = jnp.broadcast_to(
        jnp.sum(normed.astype(f32) * router_row, axis=1, keepdims=True), (cap, 128)
    )

    def logit_part(j):
        return remote(pmsg, prec.at[j], p_s.at[j], p_r.at[j], tensor=lax.rem(t + j, nt))

    def logit_copy(j):
        piece = logbuf.at[own_rows, :]
        return remote(piece, piece, l_s.at[j], l_r.at[j], seq=lax.rem(s + j, ns))

    def share_logits():
        total = pmsg[...]
        for j in range(1, nt):
            logit_part(j).wait_recv()
            total = total + prec[j]
        logbuf[own_rows, :] = total
        for j in range(1, ns):
            logit_copy(j).start()

    spread_near(1)
    spread_far(1, far)
    for j in range(1, nt):
        logit_part(j).start()

    def item(i):
        if i == 4:
            return 2, pl.ds(0, half)
        h = 1 - zhalf if i % 2 else zhalf
        return i // 2, pl.ds(pl.multiple_of(h * quarter, quarter), quarter)

    def pair(i, c):
        a, span = item(i)
        return remote(
            part.at[a, c, 1 - core, span],
            drec.at[a, c, span],
            d_s.at[i, c],
            d_r.at[i, c],
            tensor=mate,
        )

    def cross(j, i, c):
        a, span = item(i)
        return remote(
            xsnd.at[a, c, span],
            xrec.at[j, a, c, span],
            x_s.at[j - 1, i, c],
            x_r.at[j - 1, i, c],
            tensor=2 * lax.rem(x + j, nx) + core,
        )

    def emit(i, c, value):
        a, span = item(i)
        value = value.reshape(2, -1, fc)
        part[a, c, 0, span, :] = value[0]
        part[a, c, 1, span, :] = value[1]
        pair(i, c).start()

    def relay(i, c):
        a, span = item(i)
        pair(i, c).wait_recv()
        total = part[a, c, core, span, :] + drec[a, c, span, :]
        part[a, c, core, span, :] = total
        xsnd[a, c, span, :] = total.astype(bf16)
        for j in range(1, nx):
            cross(j, i, c).start()

    def cols(c):
        return pl.ds(pl.multiple_of(c * fc, fc), fc)

    def product(i, c):
        if i == 4:
            return jnp.dot(o_norm[...], wu[:, cols(c)], preferred_element_type=f32)
        span = item(i)[1]
        span_b = pl.ds(pl.multiple_of(half + span.start, quarter), quarter)
        rows_of = gathered[i // 2]
        left = jnp.concatenate([rows_of[span, :], rows_of[span_b, :]], axis=0)
        if i < 2:
            return nt_dot(left, wd[cols(c), :])
        return jnp.dot(left, wg[:, cols(c)], preferred_element_type=f32)

    def row_pass(i, start, stop, lag, before=()):
        @pl.loop(start, stop)
        def _(c):
            emit(i, c, product(i, c))
            if before:

                @pl.when(c == 0)
                def _():
                    for b in before:
                        relay(*b)

            @pl.when(c >= lag)
            def _():
                relay(i, c - lag)

    cut, cut2 = nc // 3, 2 * nc // 3
    far_a, far_b = far[: len(far) // 2], far[len(far) // 2 :]
    loads[0].wait()
    arrived_near(0)
    row_pass(0, 0, cut, 2)
    share_logits()
    row_pass(0, cut, cut2, 2)
    pass_on(0, far_a)
    row_pass(0, cut2, nc, 2)
    relay(0, nc - 2)
    pass_on(0, far_b)
    loads[1].wait()
    arrived_near(1)
    row_pass(2, 0, cut2, 3, [(0, nc - 1)])
    pass_on(1, far_a)
    row_pass(2, cut2, nc, 3)
    relay(2, nc - 3)
    arrived_far(0)
    results[4].start()
    row_pass(1, 0, cut, 2, [(2, nc - 2), (2, nc - 1)])
    pass_on(1, far_b)
    row_pass(1, cut, nc, 2)
    relay(1, nc - 2)
    loads[2].wait()
    arrived_far(1)
    results[3].start()

    @pl.loop(0, nc)
    def _(c):
        values = [product(3, c), product(4, c)]
        emit(3, c, values[0])
        emit(4, c, values[1])

        @pl.when(c == 0)
        def _():
            relay(1, nc - 1)

        @pl.when(c > 0)
        def _():
            relay(3, c - 1)
            relay(4, c - 1)

    relay(3, nc - 1)
    relay(4, nc - 1)
    for j in range(1, ns):
        logit_copy(j).wait_recv()
    rgacc[...] = jnp.zeros_like(rgacc)
    inacc[...] = jnp.zeros_like(inacc)
    acc[...] = jnp.zeros_like(acc)
    acts = (o_w, o_dg, o_du)

    def act_copy(a, c):
        piece = acts[a].at[pl.ds(mine, half), cols(c)]
        return remote(piece, piece, a_s.at[a, c], a_r.at[a, c], tensor=mate)

    def lanes(terms):
        add = terms[:, 0:128]
        for i in range(1, fc // 128):
            add = add + terms[:, i * 128 : (i + 1) * 128]
        return add

    def gate_backward(c):
        for i in range(5):
            for j in range(1, nx):
                cross(j, i, c).wait_recv()

        @pl.loop(0, half // 16)
        def _(r):
            sub = pl.ds(pl.multiple_of(r * 16, 16), 16)
            out = pl.ds(pl.multiple_of(mine + r * 16, 16), 16)
            back, gate, upper = [
                functools.reduce(
                    lambda u, v: u + v,
                    [xrec[j, a, c, sub, :].astype(f32) for j in range(1, nx)],
                    part[a, c, core, sub, :],
                )
                for a in range(3)
            ]
            logit = logbuf[out, 0:1]
            sig = jax.nn.sigmoid(gate)
            act = gate * sig
            slope = sig * (1.0 + gate * (1.0 - sig))
            hid_v = act * upper
            d_hidden = logit * back
            d_gate = (d_hidden * upper * slope).astype(bf16)
            d_up = (d_hidden * act).astype(bf16)
            o_w[out, cols(c)] = (hid_v * logit).astype(bf16)
            o_dg[out, cols(c)] = d_gate
            o_du[out, cols(c)] = d_up
            rgacc[sub, :] = rgacc[sub, :] + lanes(hid_v * back)
            inacc[sub, :] = inacc[sub, :] + lanes(
                d_gate.astype(f32) * gate + d_up.astype(f32) * upper
            )

        for a in range(3):
            act_copy(a, c).start()

    def kcols(k):
        return pl.ds(pl.multiple_of(k * kc, kc), kc)

    def back_dots(c, k):
        return nt_dot(o_dg[:, cols(c)], wg[kcols(k), cols(c)]) + nt_dot(
            o_du[:, cols(c)], wu[kcols(k), cols(c)]
        )

    def act_wait(c):
        for a in range(3):
            act_copy(a, c).wait_recv()

    def accumulate(c, start, stop):
        wide = pl.ds(start, stop - start)
        total = nt_dot(o_dg[:, cols(c)], wg[wide, cols(c)]) + nt_dot(
            o_du[:, cols(c)], wu[wide, cols(c)]
        )
        acc[:, :, wide] = acc[:, :, wide] + total.reshape(ns, cap, stop - start)

    @pl.loop(0, nc - 1)
    def _(c):
        gate_backward(c)

        @pl.when(c > 0)
        def _():
            act_wait(c - 1)
            accumulate(c - 1, 0, width // 2)
            accumulate(c - 1, width // 2, width)

    gate_backward(nc - 1)
    split = nk // 2
    rg_half = jnp.sum(rgacc[...], axis=1, keepdims=True)
    in_half = jnp.sum(inacc[...], axis=1, keepdims=True)
    in_half = in_half + rg_half * logbuf[pl.ds(mine, half), 0:1]
    first = lax.broadcasted_iota(jnp.int32, (half, 128), 1) < 64
    rgbuf[pl.ds(mine, half), :] = jnp.where(first, rg_half, in_half)
    rg_piece = rgbuf.at[pl.ds(mine, half), :]
    rg_copy = remote(rg_piece, rg_piece, rg_s, rg_r, tensor=mate)
    rg_copy.start()
    act_wait(nc - 2)
    accumulate(nc - 2, 0, split * kc)
    act_wait(nc - 1)
    for a in range(3):
        results[a].start()
    rg_copy.wait_recv()

    def ycopy(k):
        return remote(ysnd.at[k], yrec.at[k], y_s.at[k], y_r.at[k], seq=yp)

    def zcopy(j, k):
        return remote(
            zsnd.at[j, k],
            zrec.at[j, k],
            z_s.at[j - 1, k],
            z_r.at[j - 1, k],
            seq=2 * zx(j) + y,
        )

    def zstage(k):
        ycopy(k).wait_recv()
        for j in range(1, nz):
            zz = zx(j)
            zsnd[j, k] = (acc[y * nz + zz, :, kcols(k)] + yrec[k, zz].astype(f32)).astype(bf16)
            zcopy(j, k).start()
        acc[y * nz + z, :, kcols(k)] = acc[y * nz + z, :, kcols(k)] + yrec[k, z].astype(f32)

    def finish(k):
        total = back_dots(nc - 1, k) + rgbuf[:, 0:1] * router[:, kcols(k)]
        total = acc[:, :, kcols(k)] + total.reshape(ns, cap, kc)
        acc[:, :, kcols(k)] = total
        for zz in range(nz):
            ysnd[k, zz] = acc[(1 - y) * nz + zz, :, kcols(k)].astype(bf16)
        bsnd[:, kcols(k)] = jnp.sum(
            total.reshape(rows, kc) * o_norm[:, kcols(k)].astype(f32), axis=0, keepdims=True
        ) / gain[:, kcols(k)]

    def sum_y(i):
        return remote(sums[i][0], sums[i][1], gy_s.at[i], gy_r.at[i], seq=yp)

    def sum_z(i, j):
        return remote(
            sums[i][2], sums[i][3].at[j], gz_s.at[i, j], gz_r.at[i, j], seq=2 * zx(j) + y
        )

    def sum_middle(i):
        sum_y(i).wait_recv()
        sums[i][2][...] = sums[i][0][...] + sums[i][1][...]
        for j in range(1, nz):
            sum_z(i, j).start()

    def sum_end(i):
        total = sums[i][2][...]
        for j in range(1, nz):
            sum_z(i, j).wait_recv()
            total = total + sums[i][3][j]
        return total

    sums = ((asnd, ayrec, azsnd, azrec), (bsnd, byrec, bzsnd, bzrec))
    finish(0)
    ycopy(0).start()
    router_part = jnp.zeros((1, width), f32)
    for b in range(ns):
        block = o_norm[b * cap : (b + 1) * cap, :].astype(f32)
        router_part = router_part + jnp.sum(
            rgbuf[b * cap : (b + 1) * cap, 0:1] * block, axis=0, keepdims=True
        )
    asnd[:, pl.ds(0, width)] = router_part
    asnd[:, pl.ds(width, rows)] = rgbuf[...].T[64:65, :]
    asnd[:, pl.ds(width + rows, 128)] = jnp.broadcast_to(live[...].astype(f32), (1, 128))
    sum_y(0).start()
    held = max(nk - 2, 1)

    @pl.loop(1, split)
    def _(k):
        finish(k)
        ycopy(k).start()

    accumulate(nc - 2, split * kc, width)

    @pl.loop(split, held)
    def _(k):
        finish(k)
        ycopy(k).start()

    for k in range(held, nk):
        finish(k)
    sum_y(1).start()
    for k in range(held, nk):
        ycopy(k).start()
    zstage(0)
    sum_middle(0)

    @pl.loop(1, held)
    def _(k):
        zstage(k)

    sum_middle(1)
    for k in range(held, nk):
        zstage(k)
    total = sum_end(0)
    scale = lax.rsqrt(total[:, width + rows :])
    o_cs[...] = scale
    results[5].start()
    o_fin[cap : cap + 8, :] = jnp.zeros((8, width), f32)
    o_fin[cap + 1 : cap + 2, :] = total[:, 0:width] * scale[:, 0:1]
    here = (y * nz + z) * cap + lax.broadcasted_iota(jnp.int32, (cap, rows), 0)
    pick = here == lax.broadcasted_iota(jnp.int32, (cap, rows), 1)
    inner = jnp.sum(
        jnp.where(pick, total[:, width : width + rows], 0.0), axis=1, keepdims=True
    )
    inner = inner / width_total
    inverse = invbuf[:, 0:1]
    alive = (lax.broadcasted_iota(jnp.int32, (cap, 1), 0) < live[...]).astype(f32)
    o_fin[cap : cap + 1, :] = sum_end(1) * scale[:, 0:1]

    @pl.loop(0, nk)
    def _(k):
        d_normed = acc[y * nz + z, :, kcols(k)]
        for j in range(1, nz):
            zcopy(j, k).wait_recv()
            d_normed = d_normed + zrec[j, k].astype(f32)
        scaled = own[:, kcols(k)] * inverse
        o_fin[0:cap, kcols(k)] = (
            inverse * (d_normed * gain[:, kcols(k)] - scaled * inner) * alive
        )

    results[6].start()
    for m in range(2):
        agy_own(m).wait_send()
        for j in near:
            agz(m, j).wait_send()
            agd(m, j).wait_send()
        for j in far:
            agf(m, j).wait_send()
            agy(m, j).wait_send()
    for j in range(1, nt):
        square_copy(j).wait_send()
        logit_part(j).wait_send()
    for j in range(1, ns):
        logit_copy(j).wait_send()
    for i in range(2):
        sum_y(i).wait_send()
        for j in range(1, nz):
            sum_z(i, j).wait_send()
    rg_copy.wait_send()

    @pl.loop(0, nc)
    def _(c):
        for i in range(5):
            pair(i, c).wait_send()
            for j in range(1, nx):
                cross(j, i, c).wait_send()
        for a in range(3):
            act_copy(a, c).wait_send()

    @pl.loop(0, nk)
    def _(k):
        ycopy(k).wait_send()
        for j in range(1, nz):
            zcopy(j, k).wait_send()

    for result in results:
        result.wait()


def body(
    hidden_in,
    grad_out,
    slot_tokens,
    live_counts,
    norm_gain,
    router_weight,
    gate_weight,
    up_weight,
    down_weight,
):
    ns, nt = lax.axis_size("seq"), lax.axis_size("tensor")
    cap = slot_tokens.shape[0]
    tokens, width = hidden_in.shape
    hidden = gate_weight.shape[1]
    rows, nz, nx = ns * cap, ns // 2, nt // 2
    half = rows // 2
    nc = pick_chunks(hidden, (6, 4, 3, 2))
    nk = pick_chunks(width, (8, 4, 2))
    fc, kc = hidden // nc, width // nk
    wide = width + rows + 128
    vmem = pl.BlockSpec(memory_space=pltpu.VMEM)
    hbm = pl.BlockSpec(memory_space=pl.ANY)
    dma = pltpu.SemaphoreType.DMA
    tok = slot_tokens.reshape(1, cap)
    live = live_counts.reshape(1, 1)
    gain = norm_gain.reshape(1, width)
    weighted, d_gate, d_up, normed, upstream, scale, final = pl.pallas_call(
        functools.partial(kernel, ns, nt, nc, nk),
        out_shape=[
            jax.ShapeDtypeStruct((rows, hidden), bf16),
            jax.ShapeDtypeStruct((rows, hidden), bf16),
            jax.ShapeDtypeStruct((rows, hidden), bf16),
            jax.ShapeDtypeStruct((rows, width), bf16),
            jax.ShapeDtypeStruct((rows, width), bf16),
            jax.ShapeDtypeStruct((1, 128), f32),
            jax.ShapeDtypeStruct((cap + 8, width), f32),
        ],
        in_specs=[vmem] * 6 + [hbm] * 3,
        out_specs=[hbm] * 7,
        scratch_shapes=[
            pltpu.VMEM((rows, hidden), bf16),
            pltpu.VMEM((rows, hidden), bf16),
            pltpu.VMEM((rows, hidden), bf16),
            pltpu.VMEM((rows, width), bf16),
            pltpu.VMEM((rows, width), bf16),
            pltpu.VMEM((1, 128), f32),
            pltpu.VMEM((cap + 8, width), f32),
            pltpu.VMEM((width, hidden), bf16),
            pltpu.VMEM((width, hidden), bf16),
            pltpu.VMEM((hidden, width), bf16),
            pltpu.VMEM((cap, width), f32),
            pltpu.VMEM((cap, 128), f32),
            pltpu.VMEM((cap, 128), f32),
            pltpu.VMEM((nt, cap, 128), f32),
            pltpu.VMEM((cap, 128), f32),
            pltpu.VMEM((nt, cap, 128), f32),
            pltpu.VMEM((rows, 128), f32),
            pltpu.VMEM((rows, 128), f32),
            pltpu.VMEM((half, 128), f32),
            pltpu.VMEM((half, 128), f32),
            pltpu.VMEM((3, nc, 2, half, fc), f32),
            pltpu.VMEM((3, nc, half, fc), f32),
            pltpu.VMEM((3, nc, half, fc), bf16),
            pltpu.VMEM((nx, 3, nc, half, fc), bf16),
            pltpu.VMEM((ns, cap, width), f32),
            pltpu.VMEM((nk, nz, cap, kc), bf16),
            pltpu.VMEM((nk, nz, cap, kc), bf16),
            pltpu.VMEM((nz, nk, cap, kc), bf16),
            pltpu.VMEM((nz, nk, cap, kc), bf16),
            pltpu.VMEM((1, wide), f32),
            pltpu.VMEM((1, wide), f32),
            pltpu.VMEM((1, wide), f32),
            pltpu.VMEM((nz, 1, wide), f32),
            pltpu.VMEM((1, width), f32),
            pltpu.VMEM((1, width), f32),
            pltpu.VMEM((1, width), f32),
            pltpu.VMEM((nz, 1, width), f32),
            dma((3,)),
            dma((7,)),
            dma((2, nz)),
            dma((2, nz)),
            dma((2, nz)),
            dma((2, nz)),
            dma((2, nz)),
            dma((2, nz)),
            dma((nt,)),
            dma((nt,)),
            dma((nt,)),
            dma((nt,)),
            dma((ns,)),
            dma((ns,)),
            dma((5, nc)),
            dma((5, nc)),
            dma((nx - 1, 5, nc)),
            dma((nx - 1, 5, nc)),
            dma((3, nc)),
            dma((3, nc)),
            dma,
            dma,
            dma((nk,)),
            dma((nk,)),
            dma((nz - 1, nk)),
            dma((nz - 1, nk)),
            dma((2,)),
            dma((2,)),
            dma((2, nz)),
            dma((2, nz)),
        ],
        compiler_params=pltpu.CompilerParams(
            collective_id=0, has_side_effects=True, vmem_limit_bytes=67_043_328
        ),
    )(
        hidden_in,
        grad_out,
        tok,
        live,
        gain,
        router_weight.reshape(1, width),
        gate_weight,
        up_weight,
        down_weight,
    )
    grad_gate, grad_up, grad_down, grad_in, grad_gain, grad_router = outer_products(
        normed,
        d_gate,
        d_up,
        weighted,
        upstream,
        scale,
        tok,
        grad_out,
        final,
    )
    return (
        grad_in,
        grad_gate,
        grad_up,
        grad_down,
        grad_gain.reshape(width),
        grad_router.reshape(width),
    )


def solution(mesh):
    in_specs = (
        P("seq", "tensor"),
        P("seq", "tensor"),
        P("seq"),
        P("seq"),
        P("tensor"),
        P("tensor"),
        P("tensor", "seq"),
        P("tensor", "seq"),
        P("seq", "tensor"),
    )
    out_specs = (
        P("seq", "tensor"),
        P("tensor", "seq"),
        P("tensor", "seq"),
        P("seq", "tensor"),
        P("tensor"),
        P("tensor"),
    )
    return jax.shard_map(body, mesh=mesh, in_specs=in_specs, out_specs=out_specs, check_vma=False)
```
